32 devices in a mesh: expert: 8 (over z, x), pair: 4 (over y, core).
Axes of the slice: x: 2, y: 2, z: 4, core: 2. Of those that a mesh axis runs over, the one named last changes fastest.
Arguments:
- tokens: bfloat16 [12288, 2048], P(('expert', 'pair')), may hold values from -6 to 6
- token_ids: int32 [12288], P(('expert', 'pair')), may hold values from 0 to 8191
- table: int32 [8192], replicated, may hold values from 0 to 15
- w_in: bfloat16 [16, 2048, 2048], P('expert', None, 'pair'), may hold values from -0.125 to 0.125
- w_out: bfloat16 [16, 2048, 2048], P('expert', 'pair'), may hold values from -0.125 to 0.125
Outputs:
- mixed: bfloat16 [12288, 2048], P(('expert', 'pair'))
The draws below stay inside these ranges and needn't reach their ends.
All inputs are finite; a program needn't handle non-finite values.
Results may differ from the reference program's by a relative error of at most 0.0085.
Values may be sent and summed in bfloat16 or wider, within the bound.
No kernel may reach another device: no remote copies, remote signals or barrier semaphores. Data moves between devices by JAX's collectives and lax.ppermute only.
A program may use at most 192 MiB of HBM per device.

```python
import math
import jax
import jax.numpy as jnp
import numpy as np
from jax import lax

D = 2048
H = 2048
VOCAB = 8192
TOK_DEV = 384
EXPERTS = 16
CAP = 48
TOKENS = 12288
N_EXPERT = 8
N_PAIR = 4


def touch_ends(result, stream_key, smallest, high):
    index_at = [jax.random.randint(jax.random.fold_in(stream_key, axis), (), 0, length) for axis, length in enumerate(result.shape)]
    longest = result.shape.index(max(result.shape))
    beside = index_at[:longest] + [(index_at[longest] + 1) % result.shape[longest]] + index_at[longest + 1:]
    return result.at[tuple(index_at)].set(smallest).at[tuple(beside)].set(high)


def level_of(key, dims, pieces, low, largest):
    def one(dim, shards_of):
        draws = jax.random.uniform(jax.random.fold_in(jax.random.fold_in(key, 6), dim), (shards_of,), jnp.float32, low / len(pieces), largest / len(pieces))
        return jnp.repeat(jnp.exp(draws), dims[dim] // shards_of).reshape((-1,) + (1,) * (len(dims) - dim - 1))

    gain = one(*pieces[0])
    for cut in pieces[1:]:
        gain = gain * one(*cut)
    return gain


def cumulative_ranks(number_of, lean):
    portions = [(1 << 20) // math.isqrt(grade ** lean) + 1 for grade in range(1, number_of + 1)]
    width = 1 + sum(portions) // (1 << 30)
    return np.cumsum(np.array([max(1, weight // width) for weight in portions]))


def ranked(rng, extent, amount, slope):
    table = cumulative_ranks(amount, slope)
    ticket = jax.random.randint(jax.random.fold_in(rng, 1), extent, 0, int(table[amount - 1]))
    grade = jnp.searchsorted(jnp.asarray(table, jnp.int32), ticket, side="right")
    return jax.random.permutation(jax.random.fold_in(rng, 2), amount)[grade].astype(jnp.int32)


def scatter_about(key, shape, width, reach, pieces=(), kind=jnp.bfloat16):
    array = jax.random.normal(key, shape, jnp.float32) * width
    if len(pieces) > 0:
        array = level_of(key, shape, pieces, -0.22, 0.18) * array
    return jnp.clip(array, min=-reach, max=reach).astype(kind)


def setup_inputs(seed: int = 0) -> dict:
    arg_keys = jax.random.split(jax.random.key(seed), 6)
    tokens = scatter_about(arg_keys[0], (TOKENS, D), 1.0, 6.0, ((0, 32),))
    token_ids = touch_ends(ranked(arg_keys[1], (TOKENS,), VOCAB, 2), jax.random.fold_in(arg_keys[1], 3), 0, VOCAB - 1).astype(jnp.int32)
    table = touch_ends(jax.random.randint(arg_keys[2], (VOCAB,), 0, EXPERTS), jax.random.fold_in(arg_keys[2], 1), 0, EXPERTS - 1).astype(jnp.int32)
    w_in = scatter_about(arg_keys[3], (EXPERTS, D, H), D ** -0.5, 0.125, ((0, 8), (2, 4)))
    w_out = scatter_about(arg_keys[4], (EXPERTS, H, D), H ** -0.5, 0.125, ((0, 8), (1, 4)))
    return {"tokens": tokens, "token_ids": token_ids, "table": table, "w_in": w_in, "w_out": w_out}


def reference(tokens, token_ids, table, w_in, w_out):
    blocks = N_EXPERT * N_PAIR
    quarter = H // N_PAIR
    chosen = jnp.take(table, token_ids, axis=0).astype(jnp.int32).reshape(blocks, TOK_DEV)
    hot = (chosen[:, :, None] == jnp.arange(EXPERTS, dtype=jnp.int32)[None, None, :]).astype(jnp.int32)
    earlier = jnp.cumsum(hot, axis=1) - hot
    rank = jnp.sum(earlier * hot, axis=2)
    kept = rank < CAP
    block_index = jnp.arange(blocks, dtype=jnp.int32)[:, None]
    total_slots = EXPERTS * blocks * CAP
    position = (chosen * blocks + block_index) * CAP + rank
    position = jnp.where(kept, position, total_slots).reshape(-1).astype(jnp.int32)
    buffer = jnp.zeros((total_slots, D), jnp.bfloat16).at[position].set(tokens, mode="drop")
    buffer = buffer.reshape(EXPERTS, blocks * CAP, D)

    def one_expert(items):
        rows, first, second = items
        hidden = jax.nn.relu(jnp.dot(rows, first, preferred_element_type=jnp.float32)).astype(jnp.bfloat16)
        total = jnp.zeros((rows.shape[0], D), jnp.float32)
        for index in range(N_PAIR):
            part = jnp.dot(hidden[:, index * quarter:(index + 1) * quarter],
                           second[index * quarter:(index + 1) * quarter],
                           preferred_element_type=jnp.float32).astype(jnp.bfloat16)
            total = total + lax.optimization_barrier(part).astype(jnp.float32)
        return total.astype(jnp.bfloat16)

    outputs = lax.map(one_expert, (buffer, w_in, w_out)).reshape(total_slots, D)
    safe = jnp.minimum(position, total_slots - 1).astype(jnp.int32)
    picked = jnp.take(outputs, safe, axis=0)
    mixed = jnp.where(kept.reshape(-1)[:, None], picked, jnp.zeros_like(picked))
    return mixed.astype(jnp.bfloat16)
```

```python
import functools

import jax
import jax.numpy as jnp
from jax import lax
from jax.experimental import pallas as pl
from jax.experimental.pallas import tpu as pltpu
from jax.sharding import PartitionSpec as P

MIB = 1 << 20


def route(token_ids, table, experts, slots):
    chosen = jnp.take(table, token_ids, axis=0)
    expert_hot = (chosen[:, None] == jnp.arange(experts, dtype=jnp.int32)[None, :]).astype(
        jnp.int32
    )
    earlier = jnp.cumsum(expert_hot, axis=0) - expert_hot
    rank_tok = jnp.sum(earlier * expert_hot, axis=1)
    return chosen, rank_tok, rank_tok < slots


def general(tokens, token_ids, table, w_in, w_out):
    groups = lax.axis_size("expert")
    exp_local = w_in.shape[0]
    experts = groups * exp_local
    tok_rows, width = tokens.shape
    slots = max(2, 2 * tok_rows // experts)
    quarter = w_out.shape[1]
    chosen, rank_tok, kept = route(token_ids, table, experts, slots)
    column = (chosen // exp_local * slots + rank_tok) * exp_local + chosen % exp_local
    placer = (
        (column[:, None] == jnp.arange(experts * slots, dtype=jnp.int32)[None, :]) & kept[:, None]
    ).astype(jnp.bfloat16)
    packed = jnp.einsum("ts,td->sd", placer, tokens, preferred_element_type=jnp.float32).astype(
        jnp.bfloat16
    )
    packed = packed.reshape(groups * slots, exp_local, width)
    arrived = lax.all_to_all(packed, "expert", split_axis=0, concat_axis=0, tiled=True)
    rows = arrived.shape[0]
    hidden = jax.nn.relu(
        jnp.einsum(
            "red,edh->reh",
            arrived,
            lax.all_gather(w_in, "pair", axis=2, tiled=True),
            preferred_element_type=jnp.float32,
        )
    ).astype(jnp.bfloat16)
    total = jnp.zeros((rows, exp_local, width), jnp.float32)
    piece = lax.all_gather(w_out, "pair", axis=1, tiled=True)
    for index in range(piece.shape[1] // quarter):
        cols = lax.dynamic_slice_in_dim(hidden, index * quarter, quarter, 2)
        part = jnp.einsum(
            "reh,ehd->red",
            cols,
            piece[:, index * quarter : (index + 1) * quarter],
            preferred_element_type=jnp.float32,
        ).astype(jnp.bfloat16)
        total = total + part.astype(jnp.float32)
    result = total.astype(jnp.bfloat16)
    returned = lax.all_to_all(result, "expert", split_axis=0, concat_axis=0, tiled=True)
    flat = returned.reshape(experts * slots, width)
    return jnp.dot(placer, flat, preferred_element_type=jnp.float32).astype(jnp.bfloat16)


def pack_kernel(ks, per, col_ref, tok_ref, *outs):
    tok_rows = tok_ref.shape[0]
    row = lax.broadcasted_iota(jnp.int32, (per, tok_rows), 0)
    col = jnp.broadcast_to(col_ref[...], (per, tok_rows))
    one = jnp.concatenate([(col == row + k * per).astype(jnp.float32) for k in ks], axis=0)
    got = jnp.dot(one.astype(jnp.bfloat16), tok_ref[...], preferred_element_type=jnp.float32)
    for i, out in enumerate(outs):
        out[...] = got[i * per : (i + 1) * per].astype(jnp.bfloat16)


def pack(ks, per, col, tokens):
    tok_rows, width = tokens.shape
    tile = 512
    return pl.pallas_call(
        functools.partial(pack_kernel, ks, per),
        grid=(width // tile,),
        in_specs=[
            pl.BlockSpec((1, tok_rows), lambda n: (0, 0)),
            pl.BlockSpec((tok_rows, tile), lambda n: (0, n)),
        ],
        out_specs=[pl.BlockSpec((per, tile), lambda n: (0, n)) for _ in ks],
        out_shape=[jax.ShapeDtypeStruct((per, width), jnp.bfloat16) for _ in ks],
        compiler_params=pltpu.CompilerParams(vmem_limit_bytes=12 * MIB),
        cost_estimate=pl.CostEstimate(
            flops=2 * len(ks) * per * tok_rows * width,
            bytes_accessed=2 * width * (tok_rows + len(ks) * per),
            transcendentals=0,
        ),
        name="pack",
    )(col.reshape(1, tok_rows), tokens)


def unpack_kernel(ks, per, has_prev, col_ref, *refs):
    blocks, out = refs[: len(ks)], refs[-1]
    tok_rows = out.shape[0]
    lane = lax.broadcasted_iota(jnp.int32, (tok_rows, per), 1)
    col = jnp.broadcast_to(col_ref[...], (tok_rows, per))
    acc = None
    one = jnp.concatenate([(col == lane + k * per).astype(jnp.float32) for k in ks], axis=1)
    acc = jnp.dot(
        one.astype(jnp.bfloat16),
        jnp.concatenate([b[...] for b in blocks], axis=0),
        preferred_element_type=jnp.float32,
    )
    if has_prev:
        acc = acc + refs[len(ks)][...].astype(jnp.float32)
    out[...] = acc.astype(jnp.bfloat16)


def unpack(ks, per, col, blocks, prev):
    tok_rows, width = col.shape[0], blocks[0].shape[1]
    tile = 512
    wide = pl.BlockSpec((tok_rows, tile), lambda n: (0, n))
    extra = [] if prev is None else [prev]
    return pl.pallas_call(
        functools.partial(unpack_kernel, ks, per, prev is not None),
        grid=(width // tile,),
        in_specs=[pl.BlockSpec((tok_rows, 1), lambda n: (0, 0))]
        + [pl.BlockSpec((per, tile), lambda n: (0, n)) for _ in ks]
        + [wide for _ in extra],
        out_specs=wide,
        out_shape=jax.ShapeDtypeStruct((tok_rows, width), jnp.bfloat16),
        compiler_params=pltpu.CompilerParams(vmem_limit_bytes=12 * MIB),
        cost_estimate=pl.CostEstimate(
            flops=2 * len(ks) * per * tok_rows * width,
            bytes_accessed=2 * width * (tok_rows + len(ks) * per),
            transcendentals=0,
        ),
        name="unpack",
    )(col.reshape(tok_rows, 1), *blocks, *extra)


def experts_kernel(count, slots, steps, wia, wib, woa, wob, *refs):
    blocks, outs, x, acc = refs[:count], refs[count : 2 * count], refs[-2], refs[-1]
    j = pl.program_id(1)

    @pl.when(j == 0)
    def _():
        for i, b in enumerate(blocks):
            x[i * slots : (i + 1) * slots, :] = b[0]

    def step(wi, wo, first):
        h = jnp.dot(x[...], wi[0], preferred_element_type=jnp.float32)
        h = jnp.maximum(h, 0.0).astype(jnp.bfloat16)
        part = jnp.dot(h, wo[0], preferred_element_type=jnp.float32)
        if first:
            acc[...] = part
        else:
            acc[...] += part

    half = steps // 2

    @pl.when(j == 0)
    def _():
        step(wia, woa, True)

    @pl.when((j > 0) & (j < half))
    def _():
        step(wia, woa, False)

    @pl.when(j >= half)
    def _():
        step(wib, wob, False)

    @pl.when(j == steps - 1)
    def _():
        for i, o in enumerate(outs):
            o[0] = acc[i * slots : (i + 1) * slots, :].astype(jnp.bfloat16)


def experts_call(blocks, weights):
    wia, wib, woa, wob = weights
    local, width, quarter = wia.shape
    slots = blocks[0].shape[1]
    tile = quarter // 2
    steps = 2 * quarter // tile
    half = steps // 2
    rows = len(blocks) * slots
    own = lambda j: jnp.minimum(j, half - 1)
    other = lambda j: jnp.maximum(j - half, 0)
    block = pl.BlockSpec((1, slots, width), lambda e, j: (e, 0, 0))
    return pl.pallas_call(
        functools.partial(experts_kernel, len(blocks), slots, steps),
        grid=(local, steps),
        in_specs=[
            pl.BlockSpec((1, width, tile), lambda e, j: (e, 0, own(j))),
            pl.BlockSpec((1, width, tile), lambda e, j: (e, 0, other(j))),
            pl.BlockSpec((1, tile, width), lambda e, j: (e, own(j), 0)),
            pl.BlockSpec((1, tile, width), lambda e, j: (e, other(j), 0)),
        ]
        + [block for _ in blocks],
        out_specs=[block for _ in blocks],
        out_shape=[jax.ShapeDtypeStruct(blocks[0].shape, jnp.bfloat16) for _ in blocks],
        scratch_shapes=[
            pltpu.VMEM((rows, width), jnp.bfloat16),
            pltpu.VMEM((rows, width), jnp.float32),
        ],
        compiler_params=pltpu.CompilerParams(vmem_limit_bytes=40 * MIB),
        cost_estimate=pl.CostEstimate(
            flops=8 * local * rows * width * quarter,
            bytes_accessed=2 * local * (4 * width * quarter + 2 * rows * width),
            transcendentals=0,
        ),
        name="experts",
    )(wia, wib, woa, wob, *blocks)


def pipelined(tokens, token_ids, table, w_in, w_out):
    groups, pairs = lax.axis_size("expert"), lax.axis_size("pair")
    local = w_in.shape[0]
    experts = groups * local
    tok_rows, width = tokens.shape
    slots = max(2, 2 * tok_rows // experts)
    per = local * slots
    far = pairs // 2

    def to_group(block, k):
        return lax.ppermute(block, "expert", [(g, g ^ k) for g in range(groups)])

    def to_half(block):
        return lax.ppermute(block, "pair", [(p, (p + far) % pairs) for p in range(pairs)])

    def to_core(block):
        return lax.ppermute(block, "pair", [(p, p ^ 1) for p in range(pairs)])

    weights = (w_in, to_core(w_in), w_out, to_core(w_out))
    chosen, rank_tok, kept = route(token_ids, table, experts, slots)
    offset = jnp.bitwise_xor(chosen // local, lax.axis_index("expert"))
    col = jnp.where(kept, offset * per + chosen % local * slots + rank_tok, -1)

    half = groups // 2
    order = [half, half + 2, 2, 0] if groups == 8 else list(range(0, groups, 2))
    sets = [order, [k + 1 for k in order]]
    outputs = None
    for ks in sets:
        packed = pack(ks, per, col, tokens)
        here = [b if k == 0 else to_group(b, k) for k, b in zip(ks, packed)]
        there = [to_half(b) for b in here]
        shape = (local, slots, width)
        parts = experts_call([b.reshape(shape) for b in there + here], weights)
        back = [to_half(p.reshape(per, width)) for p in parts[: len(ks)]]
        sums = [
            (a.reshape(per, width).astype(jnp.float32) + b.astype(jnp.float32)).astype(jnp.bfloat16)
            for a, b in zip(parts[len(ks) :], back)
        ]
        home = [s if k == 0 else to_group(s, k) for k, s in zip(ks, sums)]
        outputs = unpack(ks, per, col, home, outputs)
    return outputs


def on_device(tokens, token_ids, table, w_in, w_out):
    groups, pairs = lax.axis_size("expert"), lax.axis_size("pair")
    local, _, quarter = w_in.shape
    tok_rows, width = tokens.shape
    slots = max(2, 2 * tok_rows // (groups * local))
    fits = groups in (4, 8) and pairs == 4 and slots % 16 == 0
    fits = fits and tok_rows % 128 == 0 and width % 512 == 0 and quarter % 256 == 0
    form = pipelined if fits else general
    return form(tokens, token_ids, table, w_in, w_out)


def solution(mesh):
    in_specs = (
        P(("expert", "pair"), None),
        P(("expert", "pair")),
        P(),
        P("expert", None, "pair"),
        P("expert", "pair", None),
    )
    out_specs = P(("expert", "pair"), None)
    return jax.shard_map(
        on_device, mesh=mesh, in_specs=in_specs, out_specs=out_specs, check_vma=False
    )
```

```python
import functools

import jax
import jax.numpy as jnp
from jax import lax
from jax.experimental import pallas as pl
from jax.experimental.pallas import tpu as pltpu
from jax.sharding import PartitionSpec as P


MIB = 1 << 20


def route(token_ids, table, experts, slots):
    chosen = jnp.take(table, token_ids, axis=0)
    expert_hot = (chosen[:, None] == jnp.arange(experts, dtype=jnp.int32)[None, :]).astype(
        jnp.int32
    )
    earlier = jnp.cumsum(expert_hot, axis=0) - expert_hot
    rank_tok = jnp.sum(earlier * expert_hot, axis=1)
    return chosen, rank_tok, rank_tok < slots


def general(tokens, token_ids, table, w_in, w_out):
    groups = lax.axis_size("expert")
    exp_local = w_in.shape[0]
    experts = groups * exp_local
    tok_rows, width = tokens.shape
    slots = max(2, 2 * tok_rows // experts)
    quarter = w_out.shape[1]
    chosen, rank_tok, kept = route(token_ids, table, experts, slots)
    column = (chosen // exp_local * slots + rank_tok) * exp_local + chosen % exp_local
    placer = (
        (column[:, None] == jnp.arange(experts * slots, dtype=jnp.int32)[None, :]) & kept[:, None]
    ).astype(jnp.bfloat16)
    packed = jnp.einsum("ts,td->sd", placer, tokens, preferred_element_type=jnp.float32).astype(
        jnp.bfloat16
    )
    packed = packed.reshape(groups * slots, exp_local, width)
    arrived = lax.all_to_all(packed, "expert", split_axis=0, concat_axis=0, tiled=True)
    rows = arrived.shape[0]
    hidden = jax.nn.relu(
        jnp.einsum(
            "red,edh->reh",
            arrived,
            lax.all_gather(w_in, "pair", axis=2, tiled=True),
            preferred_element_type=jnp.float32,
        )
    ).astype(jnp.bfloat16)
    total = jnp.zeros((rows, exp_local, width), jnp.float32)
    piece = lax.all_gather(w_out, "pair", axis=1, tiled=True)
    for index in range(piece.shape[1] // quarter):
        cols = lax.dynamic_slice_in_dim(hidden, index * quarter, quarter, 2)
        part = jnp.einsum(
            "reh,ehd->red",
            cols,
            piece[:, index * quarter : (index + 1) * quarter],
            preferred_element_type=jnp.float32,
        ).astype(jnp.bfloat16)
        total = total + part.astype(jnp.float32)
    result = total.astype(jnp.bfloat16)
    returned = lax.all_to_all(result, "expert", split_axis=0, concat_axis=0, tiled=True)
    flat = returned.reshape(experts * slots, width)
    return jnp.dot(placer, flat, preferred_element_type=jnp.float32).astype(jnp.bfloat16)


WHOLE = pl.BlockSpec(memory_space=pltpu.VMEM)


def cost(flops, moved):
    return pl.CostEstimate(flops=flops, bytes_accessed=moved, transcendentals=0)


def write_blocks(ks, per, col_row, tok_ref, outs):
    tok_rows = tok_ref.shape[0]
    row = lax.broadcasted_iota(jnp.int32, (per, tok_rows), 0)
    col = jnp.broadcast_to(col_row, (per, tok_rows))
    one = jnp.concatenate([(col == row + k * per).astype(jnp.float32) for k in ks], axis=0)
    got = jnp.dot(one.astype(jnp.bfloat16), tok_ref[...], preferred_element_type=jnp.float32)
    for i, out in enumerate(outs):
        out[...] = got[i * per : (i + 1) * per].astype(jnp.bfloat16)


def route_kernel(ks, local, slots, me_ref, ids_ref, table_hbm, tok_hbm, row_ref, col_ref, tok_ref, *refs):
    outs, (table_ref, sems) = refs[: len(ks)], refs[len(ks) :]
    table_copy = pltpu.make_async_copy(table_hbm, table_ref, sems.at[0])
    tok_copy = pltpu.make_async_copy(tok_hbm, tok_ref, sems.at[1])
    table_copy.start()
    tok_copy.start()
    tok_rows = tok_ref.shape[0]
    lines, lanes = table_ref.shape
    shift = lanes.bit_length() - 1
    first = lax.broadcasted_iota(jnp.int32, (tok_rows, tok_rows), 0)
    second = lax.broadcasted_iota(jnp.int32, (tok_rows, tok_rows), 1)
    same = first == second
    ids_row = jnp.concatenate([ids_ref[i : i + 1, :] for i in range(ids_ref.shape[0])], axis=1)
    wide_ids = jnp.broadcast_to(ids_row.astype(jnp.float32), (tok_rows, tok_rows))
    ids = jnp.sum(jnp.where(same, wide_ids, 0.0), axis=1, keepdims=True).astype(jnp.int32)
    line = lax.broadcasted_iota(jnp.int32, (tok_rows, lines), 1)
    lane = lax.broadcasted_iota(jnp.int32, (tok_rows, lanes), 1)
    hot = (line == jnp.right_shift(ids, shift)).astype(jnp.float32).astype(jnp.bfloat16)
    table_copy.wait()
    table = table_ref[...].astype(jnp.float32).astype(jnp.bfloat16)
    found = jnp.dot(hot, table, preferred_element_type=jnp.float32)
    found = jnp.where(lane == jnp.bitwise_and(ids, lanes - 1), found, 0.0)
    chosen = jnp.sum(found, axis=1, keepdims=True).astype(jnp.int32)
    mine = lane == chosen
    before = (second < first).astype(jnp.float32).astype(jnp.bfloat16)
    earlier = jnp.dot(
        before, mine.astype(jnp.float32).astype(jnp.bfloat16), preferred_element_type=jnp.float32
    )
    rank = jnp.sum(jnp.where(mine, earlier, 0.0), axis=1, keepdims=True).astype(jnp.int32)
    offset = jnp.bitwise_xor(jnp.right_shift(chosen, local.bit_length() - 1), me_ref[0])
    inner = jnp.bitwise_and(chosen, local - 1)
    col = jnp.where(rank < slots, (offset * local + inner) * slots + rank, -1)
    col_ref[...] = col
    spread = jnp.where(same, col.astype(jnp.float32), 0.0)
    col_row = jnp.sum(spread, axis=0, keepdims=True).astype(jnp.int32)
    row_ref[...] = col_row
    tok_copy.wait()
    write_blocks(ks, local * slots, col_row, tok_ref, outs)


def route_pack(ks, local, slots, me, token_ids, table, tokens):
    tok_rows, width = tokens.shape
    per = local * slots
    lanes = 128
    lined = table.reshape(-1, lanes)
    blocks = [jax.ShapeDtypeStruct((per, width), jnp.bfloat16) for _ in ks]
    there = pl.BlockSpec(memory_space=pltpu.HBM)
    row, col, tok, *out = pl.pallas_call(
        functools.partial(route_kernel, ks, local, slots),
        in_specs=[pl.BlockSpec(memory_space=pltpu.SMEM), WHOLE, there, there],
        out_specs=[WHOLE] * (3 + len(ks)),
        out_shape=[
            jax.ShapeDtypeStruct((1, tok_rows), jnp.int32),
            jax.ShapeDtypeStruct((tok_rows, 1), jnp.int32),
            jax.ShapeDtypeStruct(tokens.shape, jnp.bfloat16),
        ]
        + blocks,
        scratch_shapes=[
            pltpu.VMEM(lined.shape, jnp.int32),
            pltpu.SemaphoreType.DMA((2,)),
        ],
        compiler_params=pltpu.CompilerParams(vmem_limit_bytes=30 * MIB),
        cost_estimate=cost(4 * len(ks) * per * tok_rows * width, 4 * width * tok_rows),
        name="route_pack",
    )(me.reshape(1), token_ids.reshape(-1, lanes), lined, tokens)
    return row, col, tok, out


def pack_kernel(ks, per, row_ref, tok_ref, *outs):
    write_blocks(ks, per, row_ref[...], tok_ref, outs)


def pack(ks, per, row, tokens):
    tok_rows, width = tokens.shape
    return pl.pallas_call(
        functools.partial(pack_kernel, ks, per),
        in_specs=[WHOLE, WHOLE],
        out_specs=[WHOLE] * len(ks),
        out_shape=[jax.ShapeDtypeStruct((per, width), jnp.bfloat16) for _ in ks],
        compiler_params=pltpu.CompilerParams(vmem_limit_bytes=8 * MIB),
        cost_estimate=cost(2 * len(ks) * per * tok_rows * width, 4 * width * tok_rows),
        name="pack",
    )(row, tokens)


def unpack_kernel(ks, per, tile, has_prev, col_ref, *refs):
    blocks, out = refs[: len(ks)], refs[-1]
    tok_rows = col_ref.shape[0]
    cut = pl.ds(pl.multiple_of(pl.program_id(0) * tile, tile), tile)
    lane = lax.broadcasted_iota(jnp.int32, (tok_rows, per), 1)
    col = jnp.broadcast_to(col_ref[...], (tok_rows, per))
    one = jnp.concatenate([(col == lane + k * per).astype(jnp.float32) for k in ks], axis=1)
    acc = jnp.dot(
        one.astype(jnp.bfloat16),
        jnp.concatenate([b[:, cut] for b in blocks], axis=0),
        preferred_element_type=jnp.float32,
    )
    if has_prev:
        acc = acc + refs[len(ks)][:, cut].astype(jnp.float32)
    out[...] = acc.astype(jnp.bfloat16)


def unpack(ks, per, col, blocks, prev):
    tok_rows, width = col.shape[0], blocks[0].shape[1]
    last = prev is not None
    tile = 1024 if last else width
    extra = [prev] if last else []
    return pl.pallas_call(
        functools.partial(unpack_kernel, ks, per, tile, last),
        grid=(width // tile,),
        in_specs=[WHOLE] * (1 + len(ks) + len(extra)),
        out_specs=pl.BlockSpec((tok_rows, tile), lambda n: (0, n)) if last else WHOLE,
        out_shape=jax.ShapeDtypeStruct((tok_rows, width), jnp.bfloat16),
        compiler_params=pltpu.CompilerParams(vmem_limit_bytes=12 * MIB),
        cost_estimate=cost(2 * len(ks) * per * tok_rows * width, 4 * width * tok_rows),
        name="unpack",
    )(col, *blocks, *extra)


def add_kernel(a, b, out):
    out[...] = (a[...].astype(jnp.float32) + b[...].astype(jnp.float32)).astype(jnp.bfloat16)


def add(a, b):
    return pl.pallas_call(
        add_kernel,
        in_specs=[WHOLE, WHOLE],
        out_specs=WHOLE,
        out_shape=jax.ShapeDtypeStruct(a.shape, jnp.bfloat16),
        compiler_params=pltpu.CompilerParams(vmem_limit_bytes=4 * MIB),
        cost_estimate=cost(a.size, 6 * a.size),
        name="add",
    )(a, b)


def experts_kernel(count, slots, tile, wia, wib, woa, wob, *refs):
    blocks, outs, x, h = refs[:count], refs[count : 2 * count], refs[-2], refs[-1]
    local, width, quarter = wia.shape
    for e in range(local):
        for i, b in enumerate(blocks):
            x[i * slots : (i + 1) * slots, :] = b[e]
        for q, w in enumerate((wia, wib)):
            g = jnp.dot(x[...], w[e], preferred_element_type=jnp.float32)
            h[:, q * quarter : (q + 1) * quarter] = jnp.maximum(g, 0.0).astype(jnp.bfloat16)

        def column(t, carry, e=e):
            c = pl.ds(pl.multiple_of(t * tile, tile), tile)
            o = jnp.dot(h[:, :quarter], woa[e, :, c], preferred_element_type=jnp.float32)
            o += jnp.dot(h[:, quarter:], wob[e, :, c], preferred_element_type=jnp.float32)
            o = o.astype(jnp.bfloat16)
            for i, out in enumerate(outs):
                out[e, :, c] = o[i * slots : (i + 1) * slots]
            return carry

        lax.fori_loop(0, width // tile, column, 0)


def experts_call(blocks, weights):
    local, width, quarter = weights[0].shape
    slots = blocks[0].shape[1]
    rows = len(blocks) * slots
    return pl.pallas_call(
        functools.partial(experts_kernel, len(blocks), slots, min(1024, width)),
        in_specs=[WHOLE] * (4 + len(blocks)),
        out_specs=[WHOLE] * len(blocks),
        out_shape=[jax.ShapeDtypeStruct(blocks[0].shape, jnp.bfloat16) for _ in blocks],
        scratch_shapes=[
            pltpu.VMEM((rows, width), jnp.bfloat16),
            pltpu.VMEM((rows, 2 * quarter), jnp.bfloat16),
        ],
        compiler_params=pltpu.CompilerParams(vmem_limit_bytes=16 * MIB),
        cost_estimate=cost(
            8 * local * rows * width * quarter, 2 * local * (4 * width * quarter + 2 * rows * width)
        ),
        name="experts",
    )(*weights, *blocks)


def hold_kernel(a, b, x, y, sems):
    copies = [pltpu.make_async_copy(a, x, sems.at[0]), pltpu.make_async_copy(b, y, sems.at[1])]
    for copy in copies:
        copy.start()
    for copy in copies:
        copy.wait()


def hold(a, b):
    there = pl.BlockSpec(memory_space=pl.ANY)
    return pl.pallas_call(
        hold_kernel,
        in_specs=[there, there],
        out_specs=[WHOLE, WHOLE],
        out_shape=[jax.ShapeDtypeStruct(v.shape, v.dtype) for v in (a, b)],
        scratch_shapes=[pltpu.SemaphoreType.DMA((2,))],
        compiler_params=pltpu.CompilerParams(vmem_limit_bytes=4 * MIB),
        cost_estimate=cost(0, 4 * (a.size + b.size)),
        name="hold",
    )(a, b)


FIRST, LATER = (2, 4, 1, 0), (3, 5, 6, 7)
NEAR = ()
SETS = {"EA": (0, 1), "EB": (2, 3), "EC": (4, 5), "ED": (6, 7)}
OUT_FIRST, OUT_LATER = (2, 3, 4, 5), (0, 1, 6, 7)


def pipelined(tokens, token_ids, table, w_in, w_out):
    groups, pairs = lax.axis_size("expert"), lax.axis_size("pair")
    local = w_in.shape[0]
    tok_rows, width = tokens.shape
    slots = max(2, 2 * tok_rows // (groups * local))
    per = local * slots
    far = pairs // 2

    def to_group(block, k):
        if k == 0:
            return block
        return lax.ppermute(block, "expert", [(g, g ^ k) for g in range(groups)])

    def to_half(block):
        return lax.ppermute(block, "pair", [(p, (p + far) % pairs) for p in range(pairs)])

    def to_core(block):
        return lax.ppermute(block, "pair", [(p, p ^ 1) for p in range(pairs)])

    theirs_in, theirs_out = to_core(w_in), to_core(w_out)
    theirs_in, theirs_out = hold(theirs_in, theirs_out)
    weights = (w_in, theirs_in, w_out, theirs_out)
    me = lax.axis_index("expert").astype(jnp.int32)
    row, col, tok, out = route_pack(FIRST, local, slots, me, token_ids, table, tokens)
    packed = dict(zip(FIRST, out))
    packed.update(zip(LATER, pack(LATER, per, row, tok)))
    here = {k: to_group(packed[k], k) for k in range(groups)}
    there = {}
    for k in range(groups):
        if k in NEAR:
            there[k] = to_group(to_half(packed[k]), k)
        else:
            there[k] = to_half(here[k])
    home = {}
    for ks in SETS.values():
        blocks = [b[k].reshape(local, slots, width) for b in (there, here) for k in ks]
        parts = [p.reshape(per, width) for p in experts_call(blocks, weights)]
        for k, theirs, ours in zip(ks, parts[: len(ks)], parts[len(ks) :]):
            back = to_half(theirs)
            home[k] = to_group(add(ours, back), k)
    part = unpack(OUT_FIRST, per, col, [home[k] for k in OUT_FIRST], None)
    return unpack(OUT_LATER, per, col, [home[k] for k in OUT_LATER], part)


def on_device(tokens, token_ids, table, w_in, w_out):
    groups, pairs = lax.axis_size("expert"), lax.axis_size("pair")
    local, _, quarter = w_in.shape
    tok_rows, width = tokens.shape
    slots = max(2, 2 * tok_rows // (groups * local))
    fits = groups == 8 and pairs == 4 and local & (local - 1) == 0 and groups * local <= 128
    fits = fits and slots % 16 == 0 and tok_rows % 128 == 0 and table.shape[0] % 1024 == 0
    fits = fits and width % 1024 == 0 and quarter % 256 == 0
    if not fits:
        return general(tokens, token_ids, table, w_in, w_out)
    return pipelined(tokens, token_ids, table, w_in, w_out)


def solution(mesh):
    in_specs = (
        P(("expert", "pair"), None),
        P(("expert", "pair")),
        P(),
        P("expert", None, "pair"),
        P("expert", "pair", None),
    )
    out_specs = P(("expert", "pair"), None)
    return jax.shard_map(
        on_device, mesh=mesh, in_specs=in_specs, out_specs=out_specs, check_vma=False
    )
```

```python
import functools

import jax
import jax.numpy as jnp
from jax import lax
from jax.experimental import pallas as pl
from jax.experimental.pallas import tpu as pltpu
from jax.sharding import PartitionSpec as P


MIB = 1 << 20


def route(token_ids, table, experts, slots):
    chosen = jnp.take(table, token_ids, axis=0)
    expert_hot = (chosen[:, None] == jnp.arange(experts, dtype=jnp.int32)[None, :]).astype(
        jnp.int32
    )
    earlier = jnp.cumsum(expert_hot, axis=0) - expert_hot
    rank_tok = jnp.sum(earlier * expert_hot, axis=1)
    return chosen, rank_tok, rank_tok < slots


def general(tokens, token_ids, table, w_in, w_out):
    groups = lax.axis_size("expert")
    exp_local = w_in.shape[0]
    experts = groups * exp_local
    tok_rows, width = tokens.shape
    slots = max(2, 2 * tok_rows // experts)
    quarter = w_out.shape[1]
    chosen, rank_tok, kept = route(token_ids, table, experts, slots)
    column = (chosen // exp_local * slots + rank_tok) * exp_local + chosen % exp_local
    placer = (
        (column[:, None] == jnp.arange(experts * slots, dtype=jnp.int32)[None, :]) & kept[:, None]
    ).astype(jnp.bfloat16)
    packed = jnp.einsum("ts,td->sd", placer, tokens, preferred_element_type=jnp.float32).astype(
        jnp.bfloat16
    )
    packed = packed.reshape(groups * slots, exp_local, width)
    arrived = lax.all_to_all(packed, "expert", split_axis=0, concat_axis=0, tiled=True)
    rows = arrived.shape[0]
    hidden = jax.nn.relu(
        jnp.einsum(
            "red,edh->reh",
            arrived,
            lax.all_gather(w_in, "pair", axis=2, tiled=True),
            preferred_element_type=jnp.float32,
        )
    ).astype(jnp.bfloat16)
    total = jnp.zeros((rows, exp_local, width), jnp.float32)
    piece = lax.all_gather(w_out, "pair", axis=1, tiled=True)
    for index in range(piece.shape[1] // quarter):
        cols = lax.dynamic_slice_in_dim(hidden, index * quarter, quarter, 2)
        part = jnp.einsum(
            "reh,ehd->red",
            cols,
            piece[:, index * quarter : (index + 1) * quarter],
            preferred_element_type=jnp.float32,
        ).astype(jnp.bfloat16)
        total = total + part.astype(jnp.float32)
    result = total.astype(jnp.bfloat16)
    returned = lax.all_to_all(result, "expert", split_axis=0, concat_axis=0, tiled=True)
    flat = returned.reshape(experts * slots, width)
    return jnp.dot(placer, flat, preferred_element_type=jnp.float32).astype(jnp.bfloat16)


WHOLE = pl.BlockSpec(memory_space=pltpu.VMEM)


def cost(flops, moved):
    return pl.CostEstimate(flops=flops, bytes_accessed=moved, transcendentals=0)


def write_blocks(ks, per, col_row, tok_ref, outs):
    tok_rows = tok_ref.shape[0]
    row = lax.broadcasted_iota(jnp.int32, (per, tok_rows), 0)
    col = jnp.broadcast_to(col_row, (per, tok_rows))
    one = jnp.concatenate([(col == row + k * per).astype(jnp.float32) for k in ks], axis=0)
    got = jnp.dot(one.astype(jnp.bfloat16), tok_ref[...], preferred_element_type=jnp.float32)
    for i, out in enumerate(outs):
        out[...] = got[i * per : (i + 1) * per].astype(jnp.bfloat16)


def route_kernel(ks, local, slots, me_ref, ids_ref, table_hbm, tok_hbm, row_ref, col_ref, tok_ref, *refs):
    outs, (table_ref, sems) = refs[: len(ks)], refs[len(ks) :]
    table_copy = pltpu.make_async_copy(table_hbm, table_ref, sems.at[0])
    tok_copy = pltpu.make_async_copy(tok_hbm, tok_ref, sems.at[1])
    table_copy.start()
    tok_copy.start()
    tok_rows = tok_ref.shape[0]
    lines, lanes = table_ref.shape
    shift = lanes.bit_length() - 1
    first = lax.broadcasted_iota(jnp.int32, (tok_rows, tok_rows), 0)
    second = lax.broadcasted_iota(jnp.int32, (tok_rows, tok_rows), 1)
    same = first == second
    ids_row = jnp.concatenate([ids_ref[i : i + 1, :] for i in range(ids_ref.shape[0])], axis=1)
    wide_ids = jnp.broadcast_to(ids_row.astype(jnp.float32), (tok_rows, tok_rows))
    ids = jnp.sum(jnp.where(same, wide_ids, 0.0), axis=1, keepdims=True).astype(jnp.int32)
    line = lax.broadcasted_iota(jnp.int32, (tok_rows, lines), 1)
    lane = lax.broadcasted_iota(jnp.int32, (tok_rows, lanes), 1)
    hot = (line == jnp.right_shift(ids, shift)).astype(jnp.float32).astype(jnp.bfloat16)
    table_copy.wait()
    table = table_ref[...].astype(jnp.float32).astype(jnp.bfloat16)
    found = jnp.dot(hot, table, preferred_element_type=jnp.float32)
    found = jnp.where(lane == jnp.bitwise_and(ids, lanes - 1), found, 0.0)
    chosen = jnp.sum(found, axis=1, keepdims=True).astype(jnp.int32)
    mine = lane == chosen
    before = (second < first).astype(jnp.float32).astype(jnp.bfloat16)
    earlier = jnp.dot(
        before, mine.astype(jnp.float32).astype(jnp.bfloat16), preferred_element_type=jnp.float32
    )
    rank = jnp.sum(jnp.where(mine, earlier, 0.0), axis=1, keepdims=True).astype(jnp.int32)
    offset = jnp.bitwise_xor(jnp.right_shift(chosen, local.bit_length() - 1), me_ref[0])
    inner = jnp.bitwise_and(chosen, local - 1)
    col = jnp.where(rank < slots, (offset * local + inner) * slots + rank, -1)
    col_ref[...] = col
    spread = jnp.where(same, col.astype(jnp.float32), 0.0)
    col_row = jnp.sum(spread, axis=0, keepdims=True).astype(jnp.int32)
    row_ref[...] = col_row
    tok_copy.wait()
    write_blocks(ks, local * slots, col_row, tok_ref, outs)


def route_pack(ks, local, slots, me, token_ids, table, tokens):
    tok_rows, width = tokens.shape
    per = local * slots
    lanes = 128
    lined = table.reshape(-1, lanes)
    blocks = [jax.ShapeDtypeStruct((per, width), jnp.bfloat16) for _ in ks]
    there = pl.BlockSpec(memory_space=pltpu.HBM)
    row, col, tok, *out = pl.pallas_call(
        functools.partial(route_kernel, ks, local, slots),
        in_specs=[pl.BlockSpec(memory_space=pltpu.SMEM), WHOLE, there, there],
        out_specs=[WHOLE] * (3 + len(ks)),
        out_shape=[
            jax.ShapeDtypeStruct((1, tok_rows), jnp.int32),
            jax.ShapeDtypeStruct((tok_rows, 1), jnp.int32),
            jax.ShapeDtypeStruct(tokens.shape, jnp.bfloat16),
        ]
        + blocks,
        scratch_shapes=[
            pltpu.VMEM(lined.shape, jnp.int32),
            pltpu.SemaphoreType.DMA((2,)),
        ],
        compiler_params=pltpu.CompilerParams(vmem_limit_bytes=50 * MIB),
        cost_estimate=cost(4 * len(ks) * per * tok_rows * width, 4 * width * tok_rows),
        name="route_pack",
    )(me.reshape(1), token_ids.reshape(-1, lanes), lined, tokens)
    return row, col, tok, out


def pack_kernel(ks, per, row_ref, tok_ref, *outs):
    write_blocks(ks, per, row_ref[...], tok_ref, outs)


def pack(ks, per, row, tokens):
    tok_rows, width = tokens.shape
    return pl.pallas_call(
        functools.partial(pack_kernel, ks, per),
        in_specs=[WHOLE, WHOLE],
        out_specs=[WHOLE] * len(ks),
        out_shape=[jax.ShapeDtypeStruct((per, width), jnp.bfloat16) for _ in ks],
        compiler_params=pltpu.CompilerParams(vmem_limit_bytes=8 * MIB),
        cost_estimate=cost(2 * len(ks) * per * tok_rows * width, 4 * width * tok_rows),
        name="pack",
    )(row, tokens)


def unpack_kernel(ks, pairs, per, tile, has_prev, col_ref, *refs):
    single, out = len(ks) - pairs, refs[-1]
    count = single + 2 * pairs
    tok_rows = col_ref.shape[0]
    cut = pl.ds(pl.multiple_of(pl.program_id(0) * tile, tile), tile)
    lane = lax.broadcasted_iota(jnp.int32, (tok_rows, per), 1)
    col = jnp.broadcast_to(col_ref[...], (tok_rows, per))
    one = jnp.concatenate([(col == lane + k * per).astype(jnp.float32) for k in ks], axis=1)
    blocks = [b[:, cut] for b in refs[:single]]
    for i in range(single, count, 2):
        total = refs[i][:, cut].astype(jnp.float32) + refs[i + 1][:, cut].astype(jnp.float32)
        blocks.append(total.astype(jnp.bfloat16))
    acc = jnp.dot(
        one.astype(jnp.bfloat16),
        jnp.concatenate(blocks, axis=0),
        preferred_element_type=jnp.float32,
    )
    if has_prev:
        acc = acc + refs[count][:, cut].astype(jnp.float32)
    out[...] = acc.astype(jnp.bfloat16)


def unpack(ks, per, col, home, prev):
    ks = sorted(ks, key=lambda k: len(home[k]))
    blocks = [b for k in ks for b in home[k]]
    pairs = len(blocks) - len(ks)
    tok_rows, width = col.shape[0], blocks[0].shape[1]
    last = prev is not None
    tile = 1024 if last else width
    extra = [prev] if last else []
    return pl.pallas_call(
        functools.partial(unpack_kernel, ks, pairs, per, tile, last),
        grid=(width // tile,),
        in_specs=[WHOLE] * (1 + len(blocks) + len(extra)),
        out_specs=pl.BlockSpec((tok_rows, tile), lambda n: (0, n)) if last else WHOLE,
        out_shape=jax.ShapeDtypeStruct((tok_rows, width), jnp.bfloat16),
        compiler_params=pltpu.CompilerParams(vmem_limit_bytes=12 * MIB),
        cost_estimate=cost(2 * len(ks) * per * tok_rows * width, 4 * width * tok_rows),
        name="unpack",
    )(col, *blocks, *extra)


def add_kernel(a, b, out):
    out[...] = (a[...].astype(jnp.float32) + b[...].astype(jnp.float32)).astype(jnp.bfloat16)


def add(a, b):
    return pl.pallas_call(
        add_kernel,
        in_specs=[WHOLE, WHOLE],
        out_specs=WHOLE,
        out_shape=jax.ShapeDtypeStruct(a.shape, jnp.bfloat16),
        compiler_params=pltpu.CompilerParams(vmem_limit_bytes=4 * MIB),
        cost_estimate=cost(a.size, 6 * a.size),
        name="add",
    )(a, b)


def experts_kernel(count, slots, tile, wia, wib, woa, wob, *refs):
    blocks, outs, x, h = refs[:count], refs[count : 2 * count], refs[-2], refs[-1]
    local, width, quarter = wia.shape
    for e in range(local):
        for i, b in enumerate(blocks):
            x[i * slots : (i + 1) * slots, :] = b[e]
        for q, w in enumerate((wia, wib)):
            g = jnp.dot(x[...], w[e], preferred_element_type=jnp.float32)
            h[:, q * quarter : (q + 1) * quarter] = jnp.maximum(g, 0.0).astype(jnp.bfloat16)

        def column(t, carry, e=e):
            c = pl.ds(pl.multiple_of(t * tile, tile), tile)
            o = jnp.dot(h[:, :quarter], woa[e, :, c], preferred_element_type=jnp.float32)
            o += jnp.dot(h[:, quarter:], wob[e, :, c], preferred_element_type=jnp.float32)
            o = o.astype(jnp.bfloat16)
            for i, out in enumerate(outs):
                out[e, :, c] = o[i * slots : (i + 1) * slots]
            return carry

        lax.fori_loop(0, width // tile, column, 0)


def experts_call(blocks, weights):
    local, width, quarter = weights[0].shape
    slots = blocks[0].shape[1]
    rows = len(blocks) * slots
    return pl.pallas_call(
        functools.partial(experts_kernel, len(blocks), slots, min(1024, width)),
        in_specs=[WHOLE] * (4 + len(blocks)),
        out_specs=[WHOLE] * len(blocks),
        out_shape=[jax.ShapeDtypeStruct(blocks[0].shape, jnp.bfloat16) for _ in blocks],
        scratch_shapes=[
            pltpu.VMEM((rows, width), jnp.bfloat16),
            pltpu.VMEM((rows, 2 * quarter), jnp.bfloat16),
        ],
        compiler_params=pltpu.CompilerParams(vmem_limit_bytes=16 * MIB),
        cost_estimate=cost(
            8 * local * rows * width * quarter, 2 * local * (4 * width * quarter + 2 * rows * width)
        ),
        name="experts",
    )(*weights, *blocks)


def hold_kernel(a, b, x, y, sems):
    copies = [pltpu.make_async_copy(a, x, sems.at[0]), pltpu.make_async_copy(b, y, sems.at[1])]
    for copy in copies:
        copy.start()
    for copy in copies:
        copy.wait()


def hold(a, b):
    there = pl.BlockSpec(memory_space=pl.ANY)
    return pl.pallas_call(
        hold_kernel,
        in_specs=[there, there],
        out_specs=[WHOLE, WHOLE],
        out_shape=[jax.ShapeDtypeStruct(v.shape, v.dtype) for v in (a, b)],
        scratch_shapes=[pltpu.SemaphoreType.DMA((2,))],
        compiler_params=pltpu.CompilerParams(vmem_limit_bytes=4 * MIB),
        cost_estimate=cost(0, 4 * (a.size + b.size)),
        name="hold",
    )(a, b)


FIRST, LATER = (2, 4, 1, 0), (3, 5, 6, 7)
NEAR = ()
LATE = (0, 1)
SETS = {"EA": (0, 1), "EC": (4, 5), "EB": (2, 6), "ED": (3, 7)}
OUT_FIRST, OUT_LATER = (2, 3, 4, 5, 6, 7), (0, 1)


def pipelined(tokens, token_ids, table, w_in, w_out):
    groups, pairs = lax.axis_size("expert"), lax.axis_size("pair")
    local = w_in.shape[0]
    tok_rows, width = tokens.shape
    slots = max(2, 2 * tok_rows // (groups * local))
    per = local * slots
    far = pairs // 2

    def to_group(block, k):
        if k == 0:
            return block
        return lax.ppermute(block, "expert", [(g, g ^ k) for g in range(groups)])

    def to_half(block):
        return lax.ppermute(block, "pair", [(p, (p + far) % pairs) for p in range(pairs)])

    def to_core(block):
        return lax.ppermute(block, "pair", [(p, p ^ 1) for p in range(pairs)])

    theirs_in, theirs_out = to_core(w_in), to_core(w_out)
    theirs_in, theirs_out = hold(theirs_in, theirs_out)
    weights = (w_in, theirs_in, w_out, theirs_out)
    me = lax.axis_index("expert").astype(jnp.int32)
    row, col, tok, out = route_pack(FIRST, local, slots, me, token_ids, table, tokens)
    packed = dict(zip(FIRST, out))
    packed.update(zip(LATER, pack(LATER, per, row, tok)))
    here = {k: to_group(packed[k], k) for k in range(groups)}
    there = {}
    for k in range(groups):
        if k in NEAR:
            there[k] = to_group(to_half(packed[k]), k)
        else:
            there[k] = to_half(here[k])
    home = {}
    for ks in SETS.values():
        blocks = [b[k].reshape(local, slots, width) for b in (there, here) for k in ks]
        parts = [p.reshape(per, width) for p in experts_call(blocks, weights)]
        for k, theirs, ours in zip(ks, parts[: len(ks)], parts[len(ks) :]):
            if k in LATE:
                back = to_half(to_group(theirs, k))
                home[k] = (to_group(ours, k), back)
            else:
                home[k] = (to_group(add(ours, to_half(theirs)), k),)
    part = unpack(OUT_FIRST, per, col, home, None)
    return unpack(OUT_LATER, per, col, home, part)


def on_device(tokens, token_ids, table, w_in, w_out):
    groups, pairs = lax.axis_size("expert"), lax.axis_size("pair")
    local, _, quarter = w_in.shape
    tok_rows, width = tokens.shape
    slots = max(2, 2 * tok_rows // (groups * local))
    fits = groups == 8 and pairs == 4 and local & (local - 1) == 0 and groups * local <= 128
    fits = fits and slots % 16 == 0 and tok_rows % 128 == 0 and table.shape[0] % 1024 == 0
    fits = fits and width % 1024 == 0 and quarter % 256 == 0
    if not fits:
        return general(tokens, token_ids, table, w_in, w_out)
    return pipelined(tokens, token_ids, table, w_in, w_out)


def solution(mesh):
    in_specs = (
        P(("expert", "pair"), None),
        P(("expert", "pair")),
        P(),
        P("expert", None, "pair"),
        P("expert", "pair", None),
    )
    out_specs = P(("expert", "pair"), None)
    return jax.shard_map(
        on_device, mesh=mesh, in_specs=in_specs, out_specs=out_specs, check_vma=False
    )
```
